32 devices in a mesh: gz: 8 (over z, y), xy: 4 (over x, core).
Axes of the slice: x: 2, y: 2, z: 4, core: 2. Of those that a mesh axis runs over, the one named last changes fastest.
Arguments:
- image: float32 [64, 512, 512], P('gz', 'xy'), may hold values from -6 to 6
- offsets: int32 [4, 64, 4, 4], P(None, 'gz', 'xy'), may hold values from -6 to 6
- frac_index: int32 [4, 64, 4, 4], P(None, 'gz', 'xy'), may hold values from 0 to 15
- fractions: float32 [16, 3], replicated, may hold values from 0 to 1
Outputs:
- transported: float32 [64, 512, 512], P('gz', 'xy')
The draws below stay inside these ranges and needn't reach their ends.
All inputs are finite; a program needn't handle non-finite values.
Results may differ from the reference program's by a relative error of at most 0.0003.
Values sent between devices are 32-bit elements; how exact they have to be, the bound alone decides.
A program may use at most 128 MiB of HBM per device.

```python
import jax
import jax.numpy as jnp
from jax import lax

BLOCK = 128
NBY = 4
STEPS = 4
FRACS = 16
NX = 512
NY = 512
NZ = 64


def place_ends(values, rng, least, top_value):
    spot = [jax.random.randint(jax.random.fold_in(rng, axis), (), 0, length) for axis, length in enumerate(values.shape)]
    widest = values.shape.index(max(values.shape))
    neighbour = spot[:widest] + [(spot[widest] + 1) % values.shape[widest]] + spot[widest + 1:]
    return values.at[tuple(spot)].set(least).at[tuple(neighbour)].set(top_value)


def block_levels(own_key, shape, cuts, low, largest):
    def one(axis_at, blocks):
        draws = jax.random.uniform(jax.random.fold_in(jax.random.fold_in(own_key, 6), axis_at), (blocks,), jnp.float32, low / len(cuts), largest / len(cuts))
        return jnp.repeat(jnp.exp(draws), shape[axis_at] // blocks).reshape((-1,) + (1,) * (len(shape) - axis_at - 1))

    loudness = one(*cuts[0])
    for cut in cuts[1:]:
        loudness = loudness * one(*cut)
    return loudness


def gaussian(stream_key, shape, width, limit, pieces=(), kind=jnp.bfloat16):
    values = jax.random.normal(stream_key, shape, jnp.float32) * width
    if len(pieces) > 0:
        values = block_levels(stream_key, shape, pieces, -0.22, 0.18) * values
    return jnp.clip(values, min=-limit, max=limit).astype(kind)


def setup_inputs(seed: int = 0) -> dict:
    key_list = jax.random.split(jax.random.key(seed), 5)
    return {
        "image": gaussian(key_list[0], (NZ, NX, NY), 1.0, 6.0, ((0, 8), (1, 4)), jnp.float32),
        "offsets": place_ends(jax.random.randint(key_list[1], (STEPS, NZ, NX // BLOCK, NBY), -6, 7), jax.random.fold_in(key_list[1], 1), -6, 6).astype(jnp.int32),
        "frac_index": place_ends(jax.random.randint(key_list[2], (STEPS, NZ, NX // BLOCK, NBY), 0, FRACS), jax.random.fold_in(key_list[2], 1), 0, FRACS - 1).astype(jnp.int32),
        "fractions": jnp.clip(jax.random.uniform(key_list[3], (FRACS, 3), jnp.float32, 0.0, 1.0), 0.0, 1.0),
    }


def cubic_weights(shares):
    return (-shares * (shares - 1.0) * (shares - 2.0) / 6.0,
            (shares + 1.0) * (shares - 1.0) * (shares - 2.0) / 2.0,
            -(shares + 1.0) * shares * (shares - 2.0) / 2.0,
            (shares + 1.0) * shares * (shares - 1.0) / 6.0)


def reference(image, offsets, frac_index, fractions):
    current = image
    block_rows = NX // BLOCK
    levels = jnp.arange(NZ, dtype=jnp.int32)
    for step_index in range(STEPS):
        padded = jnp.pad(current, ((0, 0), (2, 2), (2, 2)), mode="wrap")
        shifts_all = offsets[step_index]
        index_all = frac_index[step_index]

        def one_block(block_id):
            row_index = block_id // NBY
            col_index = block_id % NBY
            sub_volume = lax.dynamic_slice(padded, (jnp.int32(0), row_index * BLOCK, col_index * BLOCK), (NZ, BLOCK + 4, BLOCK + 4))
            shifts_now = shifts_all[:, row_index, col_index]
            picked = fractions[index_all[:, row_index, col_index]]
            zweights = cubic_weights(1.0 - picked[:, 0])
            xweights = cubic_weights(1.0 - picked[:, 1])
            yweights = cubic_weights(1.0 - picked[:, 2])
            merged = jnp.zeros((NZ, BLOCK + 4, BLOCK + 4), jnp.float32)
            for node in range(4):
                source = jnp.mod(levels - shifts_now - 2 + node, NZ).astype(jnp.int32)
                merged = merged + zweights[node][:, None, None] * sub_volume[source]
            along_y = jnp.zeros((NZ, BLOCK + 4, BLOCK), jnp.float32)
            for node in range(4):
                along_y = along_y + yweights[node][:, None, None] * merged[:, :, node:node + BLOCK]
            along_x = jnp.zeros((NZ, BLOCK, BLOCK), jnp.float32)
            for node in range(4):
                along_x = along_x + xweights[node][:, None, None] * along_y[:, node:node + BLOCK, :]
            return along_x

        blocks = lax.map(one_block, jnp.arange(block_rows * NBY, dtype=jnp.int32))
        current = blocks.reshape(block_rows, NBY, NZ, BLOCK, BLOCK).transpose(2, 0, 3, 1, 4).reshape(NZ, NX, NY)
    return current
```

```python
import functools

import jax
import jax.numpy as jnp
from jax import lax
from jax.experimental import pallas as pl
from jax.experimental.pallas import tpu as pltpu
from jax.sharding import PartitionSpec as P

MESH = pl.DeviceIdType.MESH
LANES = 128


def slot_of(g, n):
    if n % 2:
        return g
    far, near = g // 2, g % 2
    return far + near * (n - 1 - 2 * far)


def device_at(slot, n):
    if n % 2:
        return slot
    half = slot // (n // 2)
    return 2 * (slot + half * (n - 1 - 2 * slot)) + half


def fused_kernel(
    n, n_xy, steps, order,
    image_ref, meta_ref, table_ref, out_ref, meta_all_ref,
    landed, cells_a, cells_b, final, send_high, send_low, recv_high, recv_low, meta_s,
    in_send, in_recv, meta_send, meta_recv, halo_send, halo_recv, out_send, out_recv, local_sem,
):
    planes = image_ref.shape[0]
    nz = n * planes
    rows = final.shape[1]
    blocks = final.shape[2] // LANES
    me = lax.axis_index("gz")
    xy = lax.axis_index("xy")
    slot = slot_of(me, n)
    line = xy * n + slot
    after = lax.rem(line + 1, n * n_xy)
    before = lax.rem(line + n * n_xy - 1, n * n_xy)
    next_id = (device_at(lax.rem(after, n), n), after // n)
    prev_id = (device_at(lax.rem(before, n), n), before // n)

    barrier = pltpu.get_barrier_semaphore()
    for i in range(1, n):
        pl.semaphore_signal(barrier, inc=1, device_id=(lax.rem(me + i, n), xy), device_id_type=MESH)
    for neighbour in (next_id, prev_id):
        pl.semaphore_signal(barrier, inc=1, device_id=neighbour, device_id_type=MESH)
    pl.semaphore_wait(barrier, n + 1)

    def meta_copy(i, owner, to):
        return pltpu.make_async_remote_copy(
            src_ref=meta_ref, dst_ref=meta_all_ref.at[pl.ds(pl.multiple_of(owner * 8, 8), 8)],
            send_sem=meta_send.at[i], recv_sem=meta_recv.at[i], device_id=(to, xy), device_id_type=MESH)

    def in_copy(i, owner, to):
        return pltpu.make_async_remote_copy(
            src_ref=image_ref.at[:, pl.ds(pl.multiple_of(slot_of(to, n) * rows, 8), rows)],
            dst_ref=landed.at[pl.ds(owner * planes, planes)],
            send_sem=in_send.at[i], recv_sem=in_recv.at[i], device_id=(to, xy), device_id_type=MESH)

    def out_copy(i, to, owner_slot):
        return pltpu.make_async_remote_copy(
            src_ref=final.at[pl.ds(to * planes, planes)],
            dst_ref=out_ref.at[:, pl.ds(pl.multiple_of(owner_slot * rows, 8), rows)],
            send_sem=out_send.at[i], recv_sem=out_recv.at[i], device_id=(to, xy), device_id_type=MESH)

    for i in order:
        to = lax.rem(me + i, n)
        meta_copy(i, me, to).start()
        in_copy(i, me, to).start()
    own_meta = pltpu.make_async_copy(
        meta_ref, meta_all_ref.at[pl.ds(pl.multiple_of(me * 8, 8), 8)], local_sem.at[0])
    own_in = pltpu.make_async_copy(
        image_ref.at[:, pl.ds(pl.multiple_of(slot * rows, 8), rows)],
        landed.at[pl.ds(me * planes, planes)], local_sem.at[1])
    own_meta.start()
    own_in.start()
    own_meta.wait()
    for i in order:
        meta_copy(i, lax.rem(me - i + n, n), lax.rem(me + i, n)).wait()
    to_scalar = pltpu.make_async_copy(meta_all_ref, meta_s, local_sem.at[2])
    to_scalar.start()
    to_scalar.wait()
    own_in.wait()
    for i in order:
        in_copy(i, lax.rem(me - i + n, n), lax.rem(me + i, n)).wait()

    def halo_copies(s, group):
        part = pl.ds(group * planes, planes)
        return (
            pltpu.make_async_remote_copy(
                src_ref=send_high.at[s, part], dst_ref=recv_high.at[s, part],
                send_sem=halo_send.at[s, 0, group], recv_sem=halo_recv.at[s, 0, group],
                device_id=next_id, device_id_type=MESH),
            pltpu.make_async_remote_copy(
                src_ref=send_low.at[s, part], dst_ref=recv_low.at[s, part],
                send_sem=halo_send.at[s, 1, group], recv_sem=halo_recv.at[s, 1, group],
                device_id=prev_id, device_id_type=MESH),
        )

    def edges(s, k, b, value):
        send_high[s, k, pl.ds(2 * b, 2), :] = value[rows - 2 : rows]
        send_low[s, k, pl.ds(b, 1), :] = value[0:1]

    @pl.loop(0, n)
    def _(group):
        @pl.loop(0, planes)
        def _(inner):
            k = group * planes + inner
            for b in range(blocks):
                value = landed[k, :, pl.ds(b * LANES, LANES)]
                cells_a[k, b, pl.ds(2, rows), :] = value
                edges(0, k, b, value)
        for copy in halo_copies(0, group):
            copy.start()

    tall = cells_a.shape[2]
    lane = lax.broadcasted_iota(jnp.int32, (tall, LANES), 1)
    left = lane >= LANES // 2
    last_two = lane >= LANES - 2
    last_one = lane >= LANES - 1
    first = lane < 1

    for s in range(steps):
        source, target = (cells_a, cells_b) if s % 2 == 0 else (cells_b, cells_a)

        @pl.loop(0, n)
        def _(group):
            for copy in halo_copies(s, group):
                copy.wait()

        @pl.loop(0, nz)
        def _(k):
            for b in range(blocks):
                source[k, b, pl.ds(0, 2), :] = recv_high[s, k, pl.ds(2 * b, 2), :]
                source[k, b, pl.ds(rows + 2, 1), :] = recv_low[s, k, pl.ds(b, 1), :]

        def plane(group, inner):
            k = group * planes + inner
            for b in range(blocks):
                spot = (s * planes + inner) * blocks + b
                shift = meta_s[group * 8, spot]
                row = meta_s[group * 8 + 1, spot]
                weight = [table_ref[row, j] for j in range(12)]
                merged = None
                rim = None
                for node in range(4):
                    at = k - shift - 2 + node + 2 * nz
                    at = jnp.bitwise_and(at, nz - 1) if nz & (nz - 1) == 0 else lax.rem(at, nz)
                    own = weight[node] * source[at, b]
                    side = weight[node] * jnp.where(
                        left, source[at, (b - 1) % blocks], source[at, (b + 1) % blocks])
                    merged = own if merged is None else merged + own
                    rim = side if rim is None else rim + side
                along = (
                    weight[8] * pltpu.roll(jnp.where(last_two, rim, merged), 2, 1)
                    + weight[9] * pltpu.roll(jnp.where(last_one, rim, merged), 1, 1)
                    + weight[10] * merged
                    + weight[11] * pltpu.roll(jnp.where(first, rim, merged), LANES - 1, 1)
                )
                value = weight[4] * along[0:rows]
                for node in range(1, 4):
                    value = value + weight[4 + node] * along[node : node + rows]
                if s < steps - 1:
                    target[k, b, pl.ds(2, rows), :] = value
                    edges(s + 1, k, b, value)
                else:
                    final[k, :, pl.ds(b * LANES, LANES)] = value

        if s < steps - 1:
            @pl.loop(0, n)
            def _(group):
                @pl.loop(0, planes)
                def _(inner):
                    plane(group, inner)
                for copy in halo_copies(s + 1, group):
                    copy.start()
        else:
            @pl.loop(1, n)
            def _(i):
                to = lax.rem(me + i, n)
                @pl.loop(0, planes)
                def _(inner):
                    plane(to, inner)
                out_copy(i, to, slot).start()
            @pl.loop(0, planes)
            def _(inner):
                plane(me, inner)

    own_out = pltpu.make_async_copy(
        final.at[pl.ds(me * planes, planes)],
        out_ref.at[:, pl.ds(pl.multiple_of(slot * rows, 8), rows)], local_sem.at[3])
    own_out.start()
    own_out.wait()
    for i in range(1, n):
        out_copy(i, lax.rem(me + i, n), slot_of(lax.rem(me - i + n, n), n)).wait()


def fused(image, offsets, frac_index, fractions, n, n_xy):
    planes, width, depth = image.shape
    steps, blocks = offsets.shape[0], offsets.shape[3]
    rows = width // n
    nz = n * planes
    length = steps * planes * blocks
    padded = -(-length // LANES) * LANES
    meta = jnp.stack([offsets.reshape(length), frac_index.reshape(length)])
    meta = jnp.pad(meta, ((0, 6), (0, padded - length)))
    columns = []
    for axis in range(3):
        columns.extend(cubic_weights(1.0 - fractions[:, axis]))
    table = jnp.stack(columns, axis=1)
    tall = -(-(rows + 3) // 8) * 8
    out, _ = pl.pallas_call(
        functools.partial(fused_kernel, n, n_xy, steps, tuple(range(1, n))),
        out_shape=(
            jax.ShapeDtypeStruct(image.shape, jnp.float32),
            jax.ShapeDtypeStruct((n * 8, padded), jnp.int32),
        ),
        in_specs=[
            pl.BlockSpec(memory_space=pl.ANY),
            pl.BlockSpec(memory_space=pl.ANY),
            pl.BlockSpec(memory_space=pltpu.SMEM),
        ],
        out_specs=(pl.BlockSpec(memory_space=pl.ANY), pl.BlockSpec(memory_space=pl.ANY)),
        scratch_shapes=[
            pltpu.VMEM((nz, rows, depth), jnp.float32),
            pltpu.VMEM((nz, blocks, tall, LANES), jnp.float32),
            pltpu.VMEM((nz, blocks, tall, LANES), jnp.float32),
            pltpu.VMEM((nz, rows, depth), jnp.float32),
            pltpu.VMEM((steps, nz, 2 * blocks, LANES), jnp.float32),
            pltpu.VMEM((steps, nz, blocks, LANES), jnp.float32),
            pltpu.VMEM((steps, nz, 2 * blocks, LANES), jnp.float32),
            pltpu.VMEM((steps, nz, blocks, LANES), jnp.float32),
            pltpu.SMEM((n * 8, padded), jnp.int32),
            pltpu.SemaphoreType.DMA((n,)),
            pltpu.SemaphoreType.DMA((n,)),
            pltpu.SemaphoreType.DMA((n,)),
            pltpu.SemaphoreType.DMA((n,)),
            pltpu.SemaphoreType.DMA((steps, 2, n)),
            pltpu.SemaphoreType.DMA((steps, 2, n)),
            pltpu.SemaphoreType.DMA((n,)),
            pltpu.SemaphoreType.DMA((n,)),
            pltpu.SemaphoreType.DMA((4,)),
        ],
        compiler_params=pltpu.CompilerParams(
            collective_id=0, has_side_effects=True, vmem_limit_bytes=48 * 1024 * 1024),
    )(image, meta, table)
    return out


def extended(cells, sides, width):
    for axis, dim in sides:
        count = lax.axis_size(axis)
        head = lax.slice_in_dim(cells, 0, width, axis=dim)
        tail = lax.slice_in_dim(cells, cells.shape[dim] - width, cells.shape[dim], axis=dim)
        cells = jnp.concatenate(
            [
                lax.ppermute(tail, axis, [(i, (i + 1) % count) for i in range(count)]),
                cells,
                lax.ppermute(head, axis, [((i + 1) % count, i) for i in range(count)]),
            ],
            axis=dim,
        )
    return cells


def cubic_weights(shares):
    return (
        -shares * (shares - 1.0) * (shares - 2.0) / 6.0,
        (shares + 1.0) * (shares - 1.0) * (shares - 2.0) / 2.0,
        -(shares + 1.0) * shares * (shares - 2.0) / 2.0,
        (shares + 1.0) * shares * (shares - 1.0) / 6.0,
    )


def column_steps(image, offsets, frac_index, fractions):
    step_count = offsets.shape[0]
    all_shifts, all_index = (
        lax.all_gather(offsets, "gz", axis=1, tiled=True),
        lax.all_gather(frac_index, "gz", axis=1, tiled=True),
    )
    standing = jnp.swapaxes(
        lax.all_to_all(image, "gz", split_axis=2, concat_axis=0, tiled=True), 1, 2
    )
    total_planes = standing.shape[0]
    width_y = standing.shape[1]
    width_x = standing.shape[2]
    column_block = lax.axis_index("gz") * width_y // width_x
    block_pick = (jnp.arange(all_shifts.shape[3], dtype=jnp.int32) == column_block).astype(
        jnp.int32
    )
    levels = jnp.arange(total_planes, dtype=jnp.int32)
    table_rows = jnp.arange(fractions.shape[0], dtype=jnp.int32)
    for step_index in range(step_count):
        shifts_now = jnp.sum(all_shifts[step_index, :, 0, :] * block_pick[None, :], axis=1)
        index_now = jnp.sum(all_index[step_index, :, 0, :] * block_pick[None, :], axis=1)
        onehot = (index_now[:, None] == table_rows[None, :]).astype(jnp.float32)
        picked = jnp.dot(onehot, fractions, precision=lax.Precision.HIGHEST)
        zweights = cubic_weights(1.0 - picked[:, 0])
        xweights = cubic_weights(1.0 - picked[:, 1])
        yweights = cubic_weights(1.0 - picked[:, 2])
        rimmed = extended(standing, (("gz", 1), ("xy", 2)), 2)
        merged = jnp.zeros(rimmed.shape, jnp.float32)
        for node in range(4):
            source = jnp.mod(levels - shifts_now - 2 + node, total_planes)
            merged = merged + zweights[node][:, None, None] * jnp.take(rimmed, source, axis=0)
        along_y = jnp.zeros((total_planes, width_y, width_x + 4), jnp.float32)
        for node in range(4):
            along_y = along_y + yweights[node][:, None, None] * merged[:, node : node + width_y, :]
        along_x = jnp.zeros((total_planes, width_y, width_x), jnp.float32)
        for node in range(4):
            along_x = along_x + xweights[node][:, None, None] * along_y[:, :, node : node + width_x]
        standing = along_x
    return lax.all_to_all(
        jnp.swapaxes(standing, 1, 2), "gz", split_axis=0, concat_axis=2, tiled=True
    )


def solution(mesh):
    n, n_xy = mesh.shape["gz"], mesh.shape["xy"]

    def local(image, offsets, frac_index, fractions):
        planes, width, depth = image.shape
        block = depth // offsets.shape[3]
        if block == width == LANES and offsets.shape[2] == 1 and width % (8 * n) == 0 and n > 1:
            return fused(image, offsets, frac_index, fractions, n, n_xy)
        return column_steps(image, offsets, frac_index, fractions)

    in_specs = (P("gz", "xy", None), P(None, "gz", "xy", None), P(None, "gz", "xy", None), P())
    out_specs = P("gz", "xy", None)
    return jax.shard_map(local, mesh=mesh, in_specs=in_specs, out_specs=out_specs, check_vma=False)
```

```python
import functools

import jax
import jax.numpy as jnp
from jax import lax
from jax.experimental import pallas as pl
from jax.experimental.pallas import tpu as pltpu
from jax.sharding import PartitionSpec as P

MESH = pl.DeviceIdType.MESH
LANES = 128


def slot_of(g, n, strip):
    if n % 2 == 0:
        far, near = g // 2, g % 2
        g = far + near * (n - 1 - 2 * far)
    return g + (strip % 2) * (n - 1 - 2 * g)


def device_at(slot, n, strip):
    slot = slot + (strip % 2) * (n - 1 - 2 * slot)
    if n % 2:
        return slot
    half = slot // (n // 2)
    return 2 * (slot + half * (n - 1 - 2 * slot)) + half


def fused_kernel(
    n, n_xy, steps,
    image_ref, meta_ref, table_ref, out_ref, meta_all_ref,
    landed, cells_a, cells_b, final, send_high, send_low, recv_high, recv_low, meta_s,
    in_send, in_recv, meta_send, meta_recv, halo_send, halo_recv, out_send, out_recv, local_sem,
):
    planes = image_ref.shape[0]
    nz = n * planes
    rows = final.shape[1]
    blocks = final.shape[2] // LANES
    pair = 2 if n_xy % 2 == 0 else 1
    pieces = n * pair
    me = lax.axis_index("gz")
    xy = lax.axis_index("xy")
    strip, half = xy // pair, lax.rem(xy, pair)
    piece = slot_of(me, n, strip) * pair + half
    home = strip * pair + piece // n
    part = lax.rem(piece, n)
    is_home = home == xy

    def holder(line):
        strip_at, piece_at = line // pieces, lax.rem(line, pieces)
        return (
            device_at(piece_at // pair, n, strip_at),
            strip_at * pair + lax.rem(piece_at, pair),
        )

    line = strip * pieces + piece
    next_id = holder(lax.rem(line + 1, n * n_xy))
    prev_id = holder(lax.rem(line + n * n_xy - 1, n * n_xy))

    barrier = pltpu.get_barrier_semaphore()
    for i in range(1, pieces):
        other = lax.rem(half * n + me + i, pieces)
        pl.semaphore_signal(
            barrier, inc=1, device_id=(lax.rem(other, n), strip * pair + other // n), device_id_type=MESH)
    for neighbour in (next_id, prev_id):
        pl.semaphore_signal(barrier, inc=1, device_id=neighbour, device_id_type=MESH)
    pl.semaphore_wait(barrier, pieces + 1)

    def share(i):
        return pl.ds(pl.multiple_of(i * rows, 8), rows)

    def slab(g):
        return pl.ds(g * planes, planes)

    def eight(g):
        return pl.ds(pl.multiple_of(g * 8, 8), 8)

    def taker(i):
        return holder(strip * pieces + half * n + i)

    def meta_copy(i):
        return pltpu.make_async_remote_copy(
            src_ref=meta_ref, dst_ref=meta_all_ref.at[eight(me)],
            send_sem=meta_send.at[i], recv_sem=meta_recv.at[me], device_id=taker(i), device_id_type=MESH)

    def in_copy(i):
        return pltpu.make_async_remote_copy(
            src_ref=image_ref.at[:, share(i)], dst_ref=landed.at[slab(me)],
            send_sem=in_send.at[i], recv_sem=in_recv.at[me], device_id=taker(i), device_id_type=MESH)

    def meta_wait(g):
        return pltpu.make_async_copy(meta_ref, meta_all_ref.at[eight(g)], meta_recv.at[g])

    def in_wait(g):
        return pltpu.make_async_copy(image_ref.at[:, share(part)], landed.at[slab(g)], in_recv.at[g])

    def out_copy(g):
        return pltpu.make_async_remote_copy(
            src_ref=final.at[slab(g)], dst_ref=out_ref.at[:, share(part)],
            send_sem=out_send.at[g], recv_sem=out_recv.at[part], device_id=(g, home), device_id_type=MESH)

    def out_wait(i):
        return pltpu.make_async_copy(final.at[slab(me)], out_ref.at[:, share(i)], out_recv.at[i])

    @pl.when(is_home)
    def _():
        meta_wait(me).start()
        in_wait(me).start()

    for make in (meta_copy, in_copy):
        @pl.loop(0, n)
        def _(turn):
            i = lax.rem(turn + me, n)

            @pl.when(jnp.logical_not(jnp.logical_and(is_home, i == part)))
            def _():
                make(i).start()

    @pl.loop(0, n)
    def _(g):
        meta_wait(g).wait()
    to_scalar = pltpu.make_async_copy(meta_all_ref, meta_s, local_sem.at[0])
    to_scalar.start()
    to_scalar.wait()

    def halo_copies(s, group):
        some = slab(group)
        return (
            pltpu.make_async_remote_copy(
                src_ref=send_high.at[s, some], dst_ref=recv_high.at[s, some],
                send_sem=halo_send.at[s, 0, group], recv_sem=halo_recv.at[s, 0, group],
                device_id=next_id, device_id_type=MESH),
            pltpu.make_async_remote_copy(
                src_ref=send_low.at[s, some], dst_ref=recv_low.at[s, some],
                send_sem=halo_send.at[s, 1, group], recv_sem=halo_recv.at[s, 1, group],
                device_id=prev_id, device_id_type=MESH),
        )

    def edges(s, k, b, value):
        send_high[s, k, pl.ds(2 * b, 2), :] = value[rows - 2 : rows]
        send_low[s, k, pl.ds(b, 1), :] = value[0:1]

    @pl.loop(0, n)
    def _(turn):
        group = lax.rem(part - turn + n, n)
        in_wait(group).wait()

        @pl.loop(0, planes, unroll=4)
        def _(inner):
            k = group * planes + inner
            for b in range(blocks):
                value = landed[k, :, pl.ds(b * LANES, LANES)]
                cells_a[k, b, pl.ds(2, rows), :] = value
                edges(0, k, b, value)
        for copy in halo_copies(0, group):
            copy.start()

    tall = cells_a.shape[2]
    lane = lax.broadcasted_iota(jnp.int32, (tall, LANES), 1)
    left = lane >= LANES // 2
    last_two = lane >= LANES - 2
    last_one = lane >= LANES - 1
    first = lane < 1

    for s in range(steps):
        source, target = (cells_a, cells_b) if s % 2 == 0 else (cells_b, cells_a)

        @pl.loop(0, n)
        def _(group):
            for copy in halo_copies(s, group):
                copy.wait_recv()

            @pl.loop(0, planes, unroll=8)
            def _(inner):
                k = group * planes + inner
                for b in range(blocks):
                    source[k, b, pl.ds(0, 2), :] = recv_high[s, k, pl.ds(2 * b, 2), :]
                    source[k, b, pl.ds(rows + 2, 1), :] = recv_low[s, k, pl.ds(b, 1), :]

        def plane(group, inner):
            k = group * planes + inner
            for b in range(blocks):
                spot = (s * planes + inner) * blocks + b
                shift = meta_s[group * 8, spot]
                row = meta_s[group * 8 + 1, spot]
                weight = [table_ref[row, j] for j in range(12)]
                merged = None
                rim = None
                for node in range(4):
                    at = k - shift - 2 + node + 2 * nz
                    at = jnp.bitwise_and(at, nz - 1) if nz & (nz - 1) == 0 else lax.rem(at, nz)
                    own = weight[node] * source[at, b]
                    side = weight[node] * jnp.where(
                        left, source[at, (b - 1) % blocks], source[at, (b + 1) % blocks])
                    merged = own if merged is None else merged + own
                    rim = side if rim is None else rim + side
                along = (
                    weight[8] * pltpu.roll(jnp.where(last_two, rim, merged), 2, 1)
                    + weight[9] * pltpu.roll(jnp.where(last_one, rim, merged), 1, 1)
                    + weight[10] * merged
                    + weight[11] * pltpu.roll(jnp.where(first, rim, merged), LANES - 1, 1)
                )
                value = weight[4] * along[0:rows]
                for node in range(1, 4):
                    value = value + weight[4 + node] * along[node : node + rows]
                if s < steps - 1:
                    target[k, b, pl.ds(2, rows), :] = value
                    edges(s + 1, k, b, value)
                else:
                    final[k, :, pl.ds(b * LANES, LANES)] = value

        if s < steps - 1:
            @pl.loop(0, n)
            def _(group):
                @pl.loop(0, planes, unroll=4)
                def _(inner):
                    plane(group, inner)
                for copy in halo_copies(s + 1, group):
                    copy.start()
        else:
            @pl.loop(0, n)
            def _(turn):
                to = lax.rem(me + turn + 1, n)

                @pl.loop(0, planes, unroll=4)
                def _(inner):
                    plane(to, inner)

                @pl.when(jnp.logical_not(jnp.logical_and(is_home, to == me)))
                def _():
                    out_copy(to).start()

    @pl.when(is_home)
    def _():
        out_wait(part).start()

    @pl.loop(0, n)
    def _(i):
        @pl.when(jnp.logical_not(jnp.logical_and(is_home, i == part)))
        def _():
            meta_copy(i).wait_send()
            in_copy(i).wait_send()

        @pl.when(jnp.logical_not(jnp.logical_and(is_home, i == me)))
        def _():
            out_copy(i).wait_send()

        out_wait(i).wait()

    for s in range(steps):
        @pl.loop(0, n)
        def _(group):
            for copy in halo_copies(s, group):
                copy.wait_send()


def fused(image, offsets, frac_index, fractions, n, n_xy):
    planes, width, depth = image.shape
    steps, blocks = offsets.shape[0], offsets.shape[3]
    rows = width // n
    nz = n * planes
    length = steps * planes * blocks
    padded = -(-length // LANES) * LANES
    meta = jnp.stack([offsets.reshape(length), frac_index.reshape(length)])
    meta = jnp.pad(meta, ((0, 6), (0, padded - length)))
    columns = []
    for axis in range(3):
        columns.extend(cubic_weights(1.0 - fractions[:, axis]))
    table = jnp.stack(columns, axis=1)
    tall = -(-(rows + 3) // 8) * 8
    out, _ = pl.pallas_call(
        functools.partial(fused_kernel, n, n_xy, steps),
        out_shape=(
            jax.ShapeDtypeStruct(image.shape, jnp.float32),
            jax.ShapeDtypeStruct((n * 8, padded), jnp.int32),
        ),
        in_specs=[
            pl.BlockSpec(memory_space=pl.ANY),
            pl.BlockSpec(memory_space=pl.ANY),
            pl.BlockSpec(memory_space=pltpu.SMEM),
        ],
        out_specs=(pl.BlockSpec(memory_space=pl.ANY), pl.BlockSpec(memory_space=pl.ANY)),
        scratch_shapes=[
            pltpu.VMEM((nz, rows, depth), jnp.float32),
            pltpu.VMEM((nz, blocks, tall, LANES), jnp.float32),
            pltpu.VMEM((nz, blocks, tall, LANES), jnp.float32),
            pltpu.VMEM((nz, rows, depth), jnp.float32),
            pltpu.VMEM((steps, nz, 2 * blocks, LANES), jnp.float32),
            pltpu.VMEM((steps, nz, blocks, LANES), jnp.float32),
            pltpu.VMEM((steps, nz, 2 * blocks, LANES), jnp.float32),
            pltpu.VMEM((steps, nz, blocks, LANES), jnp.float32),
            pltpu.SMEM((n * 8, padded), jnp.int32),
            pltpu.SemaphoreType.DMA((n,)),
            pltpu.SemaphoreType.DMA((n,)),
            pltpu.SemaphoreType.DMA((n,)),
            pltpu.SemaphoreType.DMA((n,)),
            pltpu.SemaphoreType.DMA((steps, 2, n)),
            pltpu.SemaphoreType.DMA((steps, 2, n)),
            pltpu.SemaphoreType.DMA((n,)),
            pltpu.SemaphoreType.DMA((n,)),
            pltpu.SemaphoreType.DMA((1,)),
        ],
        compiler_params=pltpu.CompilerParams(
            collective_id=0, has_side_effects=True, vmem_limit_bytes=48 * 1024 * 1024),
    )(image, meta, table)
    return out


def extended(cells, sides, width):
    for axis, dim in sides:
        count = lax.axis_size(axis)
        head = lax.slice_in_dim(cells, 0, width, axis=dim)
        tail = lax.slice_in_dim(cells, cells.shape[dim] - width, cells.shape[dim], axis=dim)
        cells = jnp.concatenate(
            [
                lax.ppermute(tail, axis, [(i, (i + 1) % count) for i in range(count)]),
                cells,
                lax.ppermute(head, axis, [((i + 1) % count, i) for i in range(count)]),
            ],
            axis=dim,
        )
    return cells


def cubic_weights(shares):
    return (
        -shares * (shares - 1.0) * (shares - 2.0) / 6.0,
        (shares + 1.0) * (shares - 1.0) * (shares - 2.0) / 2.0,
        -(shares + 1.0) * shares * (shares - 2.0) / 2.0,
        (shares + 1.0) * shares * (shares - 1.0) / 6.0,
    )


def column_steps(image, offsets, frac_index, fractions):
    step_count = offsets.shape[0]
    all_shifts, all_index = (
        lax.all_gather(offsets, "gz", axis=1, tiled=True),
        lax.all_gather(frac_index, "gz", axis=1, tiled=True),
    )
    standing = jnp.swapaxes(
        lax.all_to_all(image, "gz", split_axis=2, concat_axis=0, tiled=True), 1, 2
    )
    total_planes = standing.shape[0]
    width_y = standing.shape[1]
    width_x = standing.shape[2]
    column_block = lax.axis_index("gz") * width_y // width_x
    block_pick = (jnp.arange(all_shifts.shape[3], dtype=jnp.int32) == column_block).astype(
        jnp.int32
    )
    levels = jnp.arange(total_planes, dtype=jnp.int32)
    table_rows = jnp.arange(fractions.shape[0], dtype=jnp.int32)
    for step_index in range(step_count):
        shifts_now = jnp.sum(all_shifts[step_index, :, 0, :] * block_pick[None, :], axis=1)
        index_now = jnp.sum(all_index[step_index, :, 0, :] * block_pick[None, :], axis=1)
        onehot = (index_now[:, None] == table_rows[None, :]).astype(jnp.float32)
        picked = jnp.dot(onehot, fractions, precision=lax.Precision.HIGHEST)
        zweights = cubic_weights(1.0 - picked[:, 0])
        xweights = cubic_weights(1.0 - picked[:, 1])
        yweights = cubic_weights(1.0 - picked[:, 2])
        rimmed = extended(standing, (("gz", 1), ("xy", 2)), 2)
        merged = jnp.zeros(rimmed.shape, jnp.float32)
        for node in range(4):
            source = jnp.mod(levels - shifts_now - 2 + node, total_planes)
            merged = merged + zweights[node][:, None, None] * jnp.take(rimmed, source, axis=0)
        along_y = jnp.zeros((total_planes, width_y, width_x + 4), jnp.float32)
        for node in range(4):
            along_y = along_y + yweights[node][:, None, None] * merged[:, node : node + width_y, :]
        along_x = jnp.zeros((total_planes, width_y, width_x), jnp.float32)
        for node in range(4):
            along_x = along_x + xweights[node][:, None, None] * along_y[:, :, node : node + width_x]
        standing = along_x
    return lax.all_to_all(
        jnp.swapaxes(standing, 1, 2), "gz", split_axis=0, concat_axis=2, tiled=True
    )


def solution(mesh):
    n, n_xy = mesh.shape["gz"], mesh.shape["xy"]

    def local(image, offsets, frac_index, fractions):
        planes, width, depth = image.shape
        block = depth // offsets.shape[3]
        if block == width == LANES and offsets.shape[2] == 1 and width % (8 * n) == 0 and n > 1:
            return fused(image, offsets, frac_index, fractions, n, n_xy)
        return column_steps(image, offsets, frac_index, fractions)

    in_specs = (P("gz", "xy", None), P(None, "gz", "xy", None), P(None, "gz", "xy", None), P())
    out_specs = P("gz", "xy", None)
    return jax.shard_map(local, mesh=mesh, in_specs=in_specs, out_specs=out_specs, check_vma=False)
```
